32 devices in a mesh: dp: 2 (over y), expert: 16 (over z, x, core).
Axes of the slice: x: 2, y: 2, z: 4, core: 2. Of those that a mesh axis runs over, the one named last changes fastest.
Arguments:
- routed: bfloat16 [4096, 7168], P(('dp', 'expert')), may hold values from -160 to 160
- expert_ids: int32 [4096, 8], P(('dp', 'expert')), may hold values from 0 to 127, all different within a row
- norm_gain: bfloat16 [7168], replicated, may hold values from 0.099609375 to 1.8984375
- gate_weight: bfloat16 [16, 7168, 2048], P('expert', None, 'dp'), may hold values from -0.0625 to 0.0625
- up_weight: bfloat16 [16, 7168, 2048], P('expert', None, 'dp'), may hold values from -0.0625 to 0.0625
- down_weight: bfloat16 [16, 2048, 7168], P('expert', 'dp'), may hold values from -0.125 to 0.125
- old_place: int32 [16], replicated, may hold values from 0 to 127, as said below
- new_place: int32 [16], replicated, may hold values from 0 to 127, as said below
- probe_ids: int32 [1280], P(('dp', 'expert')), may hold values from 0 to 127
Outputs:
- expert_load: float32 [128], P('expert')
- expert_energy: float32 [128], P('expert')
- probe_out: bfloat16 [1280, 7168], P(('dp', 'expert'))
The draws below stay inside these ranges and needn't reach their ends.
Inputs may be any that keep to these rules, and one draw needn't show every extreme that they name: `old_place`: 16 different experts. `new_place`: the same 16 experts as old_place, in some order.
All inputs are finite; a program needn't handle non-finite values.
Results may differ from the reference program's by a relative error of at most 0.012.
Values may be sent and summed in bfloat16 or wider, within the bound.
A program may use at most 128 MiB of HBM per device.

```python
import jax
import jax.numpy as jnp
from jax import lax

D = 7168
FF = 2048
TOP = 8
TOK_DEV = 128
PROBE = 40
EXPERTS = 128
SLOTS = 16
TOKENS = 4096
PROBES = 1280
N_DP = 2


def draw_routed(key, part):
    first = jax.random.fold_in(key, 101)
    second = jax.random.fold_in(key, 202)
    third = jax.random.fold_in(key, 303)
    row_scale = jnp.exp(jax.random.uniform(second, (TOKENS, 1), minval=-1.15, maxval=1.15))
    column_scale = jnp.exp(jax.random.uniform(third, (1, D), minval=-1.15, maxval=1.15))
    rising = jnp.exp(jnp.log(3.0) * (jnp.arange(TOKENS, dtype=jnp.float32) / TOKENS - 0.5))[:, None]
    values = jnp.clip(jax.random.normal(first, (TOKENS, D)), -4.0, 4.0)
    return (values * row_scale * column_scale * rising).astype(jnp.bfloat16)


def draw_plan(key):
    base = jax.random.fold_in(key, 17)
    chosen = jax.random.permutation(jax.random.fold_in(base, 1), EXPERTS)[:SLOTS]
    order = jax.random.permutation(jax.random.fold_in(base, 2), SLOTS)
    return (chosen.astype(jnp.int32), jnp.take(chosen, order).astype(jnp.int32))


def draw_old_place(key, part):
    return draw_plan(key)[0]


def draw_new_place(key, part):
    return draw_plan(key)[1]


def with_ends(values, own_key, least, high):
    longest = values.shape.index(max(values.shape))
    spots = []
    for shift in (0, 1):
        where = [jax.random.randint(jax.random.fold_in(own_key, axis), (), 0, length) for axis, length in enumerate(values.shape)]
        where[longest] = (where[longest] + shift) % values.shape[longest]
        spots.append(tuple(where))
    return values.at[spots[0]].set(least).at[spots[1]].set(high)


def block_levels(stream_key, extent, pieces, low, top_value):
    level, own = 1.0, jax.random.fold_in(stream_key, 6)
    for dim, parts in pieces:
        steps = jnp.exp(jax.random.uniform(jax.random.fold_in(own, dim), (parts,), jnp.float32, low / len(pieces), top_value / len(pieces)))
        level = level * jnp.repeat(steps, extent[dim] // parts).reshape([-1 if axis == dim else 1 for axis in range(len(extent))])
    return level


def picks_of(rng, rows, count, top, lift):
    ranking = jax.random.permutation(jax.random.fold_in(rng, 1), count)
    pull = ranking
    for power in range(3):
        pull = pull * pull // count
    pull = pull * lift // count
    tickets = jax.random.randint(jax.random.fold_in(rng, 2), (rows, count), 0, 4096) + pull
    holders = jax.random.permutation(jax.random.fold_in(rng, 3), rows)[jnp.arange(count) % rows]
    tickets = jnp.where(jnp.arange(rows)[:, None] == holders[None, :], 1 << 14, tickets)
    merit = tickets * count + jnp.arange(count)
    return lax.top_k(merit.astype(jnp.int32), top)[1].astype(jnp.int32)


def noise(stream_key, shape, deviation, most, cuts=(), kind=jnp.bfloat16):
    array = deviation * jax.random.normal(stream_key, shape, jnp.float32)
    if cuts:
        array = array * block_levels(stream_key, shape, cuts, -0.22, 0.18)
    return jnp.clip(array, -most, most).astype(kind)


def setup_inputs(seed: int = 0) -> dict:
    seeds = jax.random.split(jax.random.key(seed), 10)
    return {
        "routed": draw_routed(jax.random.fold_in(seeds[9], 71), 0),
        "expert_ids": picks_of(seeds[1], TOKENS, EXPERTS, TOP, 1024),
        "norm_gain": jnp.clip(1.0 + 0.18 * jax.random.normal(seeds[2], (D,), jnp.float32), 0.099609375, 1.8984375).astype(jnp.bfloat16),
        "gate_weight": noise(seeds[3], (SLOTS, D, FF), D ** -0.5, 0.0625, ((0, 16), (2, 2))),
        "up_weight": noise(seeds[4], (SLOTS, D, FF), D ** -0.5, 0.0625, ((0, 16), (2, 2))),
        "down_weight": noise(seeds[5], (SLOTS, FF, D), FF ** -0.5, 0.125, ((0, 16), (1, 2))),
        "old_place": draw_old_place(jax.random.fold_in(seeds[9], 71), 0),
        "new_place": draw_new_place(jax.random.fold_in(seeds[9], 71), 0),
        "probe_ids": with_ends(jax.random.randint(seeds[8], (PROBES,), 0, TOK_DEV), jax.random.fold_in(seeds[8], 1), 0, TOK_DEV - 1).astype(jnp.int32),
    }


epsilon = 1e-06

def block_stats(block):
    token_rows, id_block = block
    features = token_rows.astype(jnp.float32)
    mean_square = lax.optimization_barrier(jnp.sum(features * features, axis=1)) / D
    positions = jnp.arange(EXPERTS, dtype=jnp.int32)
    onehot = lax.optimization_barrier(jnp.sum((id_block[:, :, None] == positions[None, None, :]).astype(jnp.float32), axis=1))
    columns = jnp.stack([jnp.ones_like(mean_square), mean_square])
    return (jnp.dot(columns, onehot, precision=lax.Precision.HIGHEST), mean_square)

def reference(routed, expert_ids, norm_gain, gate_weight, up_weight, down_weight, old_place, new_place, probe_ids):
    blocks = TOKENS // TOK_DEV
    stats, mean_square = lax.map(block_stats, (routed.reshape(blocks, TOK_DEV, D), expert_ids.reshape(blocks, TOK_DEV, TOP)))
    totals = lax.optimization_barrier(jnp.sum(stats, axis=0))
    counts = totals[0]
    expert_load = counts * EXPERTS / (TOKENS * TOP)
    expert_energy = totals[1] / counts
    mean_square = mean_square.reshape(TOKENS)
    offsets = jnp.arange(PROBES, dtype=jnp.int32) // PROBE * TOK_DEV
    picked = (offsets + probe_ids).astype(jnp.int32)
    picked_rows = jnp.take(routed, picked, axis=0).astype(jnp.float32)
    scale = lax.rsqrt(jnp.take(mean_square, picked) + epsilon)
    normed = (picked_rows * scale[:, None] * norm_gain.astype(jnp.float32)[None, :]).astype(jnp.bfloat16)
    grouped = normed.reshape(N_DP, SLOTS, PROBE, D)
    slot_index = jnp.arange(SLOTS, dtype=jnp.int32)
    hidden_block = FF // N_DP

    def per_slot(slot_number):
        holder = jnp.sum(jnp.where(old_place == new_place[slot_number], slot_index, 0)).astype(jnp.int32)
        inputs = lax.dynamic_index_in_dim(grouped, slot_number, 1, keepdims=False).reshape(N_DP * PROBE, D)
        gate_matrix = lax.dynamic_index_in_dim(gate_weight, holder, 0, keepdims=False)
        up_matrix = lax.dynamic_index_in_dim(up_weight, holder, 0, keepdims=False)
        down_matrix = lax.dynamic_index_in_dim(down_weight, holder, 0, keepdims=False)
        gate_value = jnp.dot(inputs, gate_matrix, preferred_element_type=jnp.float32)
        up_value = jnp.dot(inputs, up_matrix, preferred_element_type=jnp.float32)
        hidden = (jax.nn.silu(gate_value) * up_value).astype(jnp.bfloat16)
        running = jnp.zeros((N_DP * PROBE, D), jnp.float32)
        for group_index in range(N_DP):
            lower = group_index * hidden_block
            partial_value = jnp.dot(hidden[:, lower:lower + hidden_block], down_matrix[lower:lower + hidden_block], preferred_element_type=jnp.float32).astype(jnp.bfloat16)
            partial_value = lax.optimization_barrier(partial_value)
            running = running + partial_value.astype(jnp.float32)
        return running.astype(jnp.bfloat16).reshape(N_DP, PROBE, D)
    results = lax.map(per_slot, slot_index)
    probe_out = jnp.transpose(results, (1, 0, 2, 3)).reshape(PROBES, D)
    return (expert_load, expert_energy, probe_out)
```

```python
import functools

import jax
import jax.numpy as jnp
from jax import lax
from jax.experimental import pallas as pl
from jax.experimental.pallas import tpu as pltpu
from jax.sharding import PartitionSpec as P

EXP_DEV = 8
LANES = 128
MESH = pl.DeviceIdType.MESH
VMEM = pl.BlockSpec(memory_space=pltpu.VMEM)
SMEM = pl.BlockSpec(memory_space=pltpu.SMEM)
epsilon = 1e-06


def piece_width(width, n):
    w = LANES * -(-width // (LANES * n))
    while width % w:
        w += LANES
    return w


def prepare_kernel(routed, ids, probe, gain, normed, stats):
    tokens, width = routed.shape
    experts = stats.shape[1]
    total = jnp.zeros((tokens, LANES), jnp.float32)
    for c in range(width // LANES):
        x = routed[:, c * LANES : (c + 1) * LANES].astype(jnp.float32)
        total = total + x * x
    mean_square = jnp.sum(total, axis=1, keepdims=True) / width
    lane = lax.broadcasted_iota(jnp.int32, (tokens, experts), 1)
    chosen = jnp.zeros((tokens, experts), jnp.float32)
    for k in range(ids.shape[1]):
        chosen = chosen + jnp.where(ids[:, k : k + 1] == lane, 1.0, 0.0)
    stats[...] = jnp.zeros_like(stats)
    stats[0:1, :] = jnp.sum(chosen, axis=0, keepdims=True)
    stats[1:2, :] = jnp.sum(chosen * mean_square, axis=0, keepdims=True)
    probes = probe.shape[0]
    row = lax.broadcasted_iota(jnp.int32, (tokens, tokens), 0)
    column = lax.broadcasted_iota(jnp.int32, (tokens, tokens), 1)
    flat = jnp.sum(jnp.where(row == column, mean_square, 0.0), axis=0, keepdims=True)
    pick = probe[...] == lax.broadcasted_iota(jnp.int32, (probes, tokens), 1)
    scale = lax.rsqrt(jnp.sum(jnp.where(pick, flat, 0.0), axis=1, keepdims=True) + epsilon)
    pick = jnp.where(pick, 1.0, 0.0).astype(jnp.bfloat16)
    step = 512 if width % 512 == 0 else LANES
    for c in range(width // step):
        cols = slice(c * step, (c + 1) * step)
        rows = jnp.dot(pick, routed[:, cols], preferred_element_type=jnp.float32)
        normed[:, cols] = (rows * scale * gain[:, cols].astype(jnp.float32)).astype(jnp.bfloat16)


def prepare(routed, expert_ids, probe_ids, norm_gain, experts):
    probes = probe_ids.shape[0]
    width = routed.shape[1]
    return pl.pallas_call(
        prepare_kernel,
        out_shape=(
            jax.ShapeDtypeStruct((probes, width), jnp.bfloat16),
            jax.ShapeDtypeStruct((8, experts), jnp.float32),
        ),
        in_specs=[VMEM] * 4,
        out_specs=(VMEM, VMEM),
        compiler_params=pltpu.CompilerParams(vmem_limit_bytes=16 << 20),
        cost_estimate=pl.CostEstimate(flops=10**8, bytes_accessed=3 << 20, transcendentals=0),
    )(routed, expert_ids, probe_ids.reshape(probes, 1), norm_gain.reshape(1, width))


def remote(src, dst, send, recv, device):
    return pltpu.make_async_remote_copy(
        src_ref=src, dst_ref=dst, send_sem=send, recv_sem=recv, device_id=device, device_id_type=MESH
    )


def greet(g, me, d, n):
    barrier = pltpu.get_barrier_semaphore()
    for k in range(1, n):
        pl.semaphore_signal(barrier, inc=1, device_id=(g, lax.rem(me + k, n)), device_id_type=MESH)
    for c in range(1, d):
        pl.semaphore_signal(barrier, inc=1, device_id=(lax.rem(g + c, d), me), device_id_type=MESH)
    pl.semaphore_wait(barrier, n - 1 + d - 1)


class Pieces:
    def __init__(self, width, n):
        self.n = n
        self.w = piece_width(width, n)
        self.count = width // self.w

    def of(self, i):
        p = (i * self.count + self.n - 1) // self.n
        return jnp.minimum(p, self.count - 1), (p < self.count) & ((p * self.n) // self.count == i)

    def cols(self, p):
        return pl.ds(pl.multiple_of(p * self.w, self.w), self.w)


def forward_kernel(d, n, source, normed, stats, x, totals, relay, outbox, st_in, st_mid, st_dp,
                   s1, r1, s2, r2, sy, ry, ss, rs, ssy, rsy):
    g, me = lax.axis_index("dp"), lax.axis_index("expert")
    pieces = Pieces(normed.shape[1], n)
    mine, relays = pieces.of(me)
    greet(g, me, d, n)

    def first(k):
        t = lax.rem(me + k, n)
        p, ok = pieces.of(t)
        return remote(normed.at[:, pieces.cols(p)], relay.at[me], s1.at[k], r1.at[me], (g, t)), ok

    def first_in(k):
        s = lax.rem(me + n - k, n)
        return remote(normed.at[:, pieces.cols(mine)], relay.at[s], s1.at[k], r1.at[s], (g, s))

    def stat(k):
        t = lax.rem(me + k, n)
        return remote(stats, st_in.at[me], ss.at[k], rs.at[me], (g, t))

    def stat_in(k):
        s = lax.rem(me + n - k, n)
        return remote(stats, st_in.at[s], ss.at[k], rs.at[s], (g, s))

    for k in range(1, n):
        copy, ok = first(k)
        pl.when(ok)(copy.start)
    for k in range(1, n):
        stat(k).start()
    st_in[me] = stats[...]

    @pl.when(relays)
    def _():
        relay[me] = normed[:, pieces.cols(mine)]
        for k in range(1, n):
            first_in(k).wait_recv()
        for k in range(1, n):
            j = lax.rem(me + k, n)
            outbox[j] = relay[source[j]]
            remote(outbox.at[j], x.at[g, :, pieces.cols(mine)], s2.at[k], r2.at[mine], (g, j)).start()
        x[g, :, pieces.cols(mine)] = relay[source[me]]

    def along(p, c):
        here = x.at[g, :, pieces.cols(p)]
        return remote(here, here, sy.at[c, p], ry.at[g, p], (lax.rem(g + c, d), me))

    for k in range(n):
        i = lax.rem(me + n - k, n)
        p, ok = pieces.of(i)

        @pl.when(ok)
        def _():
            if k:
                remote(outbox.at[i], x.at[g, :, pieces.cols(p)], s2.at[k], r2.at[p], (g, i)).wait_recv()
            for c in range(1, d):
                along(p, c).start()

    for k in range(1, n):
        stat_in(k).wait_recv()
    mid = st_in[0]
    for s in range(1, n):
        mid = mid + st_in[s]
    st_mid[...] = mid
    st_dp[g] = mid
    for c in range(1, d):
        remote(st_mid, st_dp.at[g], ssy.at[c], rsy.at[g], (lax.rem(g + c, d), me)).start()
    for c in range(1, d):
        f = lax.rem(g + d - c, d)
        remote(st_mid, st_dp.at[f], ssy.at[c], rsy.at[f], (f, me)).wait_recv()
    total = st_dp[0]
    for f in range(1, d):
        total = total + st_dp[f]
    totals[...] = total

    for c in range(1, d):
        f = lax.rem(g + d - c, d)
        for p in range(pieces.count):
            there = x.at[f, :, pieces.cols(p)]
            remote(there, there, sy.at[c, p], ry.at[f, p], (f, me)).wait_recv()

    for k in range(1, n):
        copy, ok = first(k)
        pl.when(ok)(copy.wait_send)
        stat(k).wait_send()
    for c in range(1, d):
        remote(st_mid, st_dp.at[g], ssy.at[c], rsy.at[g], (lax.rem(g + c, d), me)).wait_send()
        for p in range(pieces.count):
            along(p, c).wait_send()

    @pl.when(relays)
    def _():
        for k in range(1, n):
            j = lax.rem(me + k, n)
            remote(outbox.at[j], x.at[g, :, pieces.cols(mine)], s2.at[k], r2.at[mine], (g, j)).wait_send()


def forward(normed, stats, source, d, n):
    rows, width = normed.shape
    pieces = Pieces(width, n)
    dma = pltpu.SemaphoreType.DMA
    return pl.pallas_call(
        functools.partial(forward_kernel, d, n),
        out_shape=(
            jax.ShapeDtypeStruct((d, rows, width), jnp.bfloat16),
            jax.ShapeDtypeStruct(stats.shape, jnp.float32),
        ),
        in_specs=[SMEM, VMEM, VMEM],
        out_specs=(VMEM, VMEM),
        scratch_shapes=[
            pltpu.VMEM((n, rows, pieces.w), jnp.bfloat16),
            pltpu.VMEM((n, rows, pieces.w), jnp.bfloat16),
            pltpu.VMEM((n,) + stats.shape, jnp.float32),
            pltpu.VMEM(stats.shape, jnp.float32),
            pltpu.VMEM((d,) + stats.shape, jnp.float32),
            dma((n,)), dma((n,)), dma((n,)), dma((pieces.count,)),
            dma((d, pieces.count)), dma((d, pieces.count)),
            dma((n,)), dma((n,)), dma((d,)), dma((d,)),
        ],
        compiler_params=pltpu.CompilerParams(
            collective_id=0, has_side_effects=True, vmem_limit_bytes=16 << 20
        ),
        cost_estimate=pl.CostEstimate(flops=10**6, bytes_accessed=100 << 20, transcendentals=0),
    )(source, normed, stats)


def back_kernel(d, n, source, partial, out, arrived, summed, relay, outbox, sy, ry, s1, r1, s2, r2):
    g, me = lax.axis_index("dp"), lax.axis_index("expert")
    pieces = Pieces(out.shape[1], n)
    mine, relays = pieces.of(me)
    greet(g, me, d, n)

    def along(p, c):
        t = lax.rem(g + c, d)
        return remote(partial.at[t, :, pieces.cols(p)], arrived.at[g, p], sy.at[c, p], ry.at[g, p], (t, me))

    def first(p, k, t):
        return remote(summed.at[p], relay.at[me], s1.at[k], r1.at[me], (g, t))

    order = [(k, lax.rem(me + k, n)) for k in range(n)]
    for k, t in order:
        p, ok = pieces.of(t)

        @pl.when(ok)
        def _():
            for c in range(1, d):
                along(p, c).start()

    for k, t in order:
        p, ok = pieces.of(t)

        @pl.when(ok)
        def _():
            for c in range(1, d):
                f = lax.rem(g + d - c, d)
                remote(partial.at[f, :, pieces.cols(p)], arrived.at[f, p], sy.at[c, p], ry.at[f, p], (f, me)).wait_recv()
            arrived[g, p] = partial[g, :, pieces.cols(p)]
            total = arrived[0, p].astype(jnp.float32)
            for f in range(1, d):
                total = total + arrived[f, p].astype(jnp.float32)
            summed[p] = total.astype(jnp.bfloat16)
            if k:
                first(p, k, t).start()
            else:
                relay[me] = total.astype(jnp.bfloat16)

    @pl.when(relays)
    def _():
        for k in range(1, n):
            s = lax.rem(me + n - k, n)
            remote(summed.at[mine], relay.at[s], s1.at[k], r1.at[s], (g, s)).wait_recv()
        for k in range(1, n):
            j = lax.rem(me + k, n)
            outbox[j] = relay[source[j]]
            remote(outbox.at[j], out.at[:, pieces.cols(mine)], s2.at[k], r2.at[mine], (g, j)).start()
        out[:, pieces.cols(mine)] = relay[source[me]]

    for k in range(1, n):
        i = lax.rem(me + n - k, n)
        p, ok = pieces.of(i)

        @pl.when(ok)
        def _():
            remote(outbox.at[i], out.at[:, pieces.cols(p)], s2.at[k], r2.at[p], (g, i)).wait_recv()

    for k, t in order:
        p, ok = pieces.of(t)

        @pl.when(ok)
        def _():
            for c in range(1, d):
                along(p, c).wait_send()
            if k:
                first(p, k, t).wait_send()

    @pl.when(relays)
    def _():
        for k in range(1, n):
            j = lax.rem(me + k, n)
            remote(outbox.at[j], out.at[:, pieces.cols(mine)], s2.at[k], r2.at[mine], (g, j)).wait_send()


def back(partial, source, n):
    d, rows, width = partial.shape
    pieces = Pieces(width, n)
    dma = pltpu.SemaphoreType.DMA
    return pl.pallas_call(
        functools.partial(back_kernel, d, n),
        out_shape=jax.ShapeDtypeStruct((rows, width), jnp.bfloat16),
        in_specs=[SMEM, VMEM],
        out_specs=VMEM,
        scratch_shapes=[
            pltpu.VMEM((d, pieces.count, rows, pieces.w), jnp.bfloat16),
            pltpu.VMEM((pieces.count, rows, pieces.w), jnp.bfloat16),
            pltpu.VMEM((n, rows, pieces.w), jnp.bfloat16),
            pltpu.VMEM((n, rows, pieces.w), jnp.bfloat16),
            dma((d, pieces.count)), dma((d, pieces.count)),
            dma((n,)), dma((n,)), dma((n,)), dma((pieces.count,)),
        ],
        compiler_params=pltpu.CompilerParams(
            collective_id=1, has_side_effects=True, vmem_limit_bytes=24 << 20
        ),
        cost_estimate=pl.CostEstimate(flops=10**6, bytes_accessed=100 << 20, transcendentals=0),
    )(source, partial)


def on_device(
    routed,
    expert_ids,
    norm_gain,
    gate_weight,
    up_weight,
    down_weight,
    old_place,
    new_place,
    probe_ids,
):
    n, d = lax.axis_size("expert"), lax.axis_size("dp")
    experts = EXP_DEV * n
    tokens = routed.shape[0] * d * n
    normed, stats = prepare(routed, expert_ids, probe_ids, norm_gain, experts)
    slot_index = jnp.arange(n, dtype=jnp.int32)
    matches = new_place[:, None] == old_place[None, :]
    sources = jnp.sum(jnp.where(matches, slot_index[None, :], 0), axis=1)
    targets = jnp.sum(jnp.where(matches, slot_index[:, None], 0), axis=0)
    x, totals = forward(normed, stats, targets, d, n)
    owned = lax.dynamic_slice_in_dim(totals, lax.axis_index("expert") * EXP_DEV, EXP_DEV, 1)
    expert_load = owned[0] * experts / (tokens * expert_ids.shape[1])
    expert_energy = owned[1] / owned[0]
    rows, width = normed.shape
    x = x.reshape(d * rows, width)
    gate_value = jnp.dot(x, gate_weight[0], preferred_element_type=jnp.float32)
    up_value = jnp.dot(x, up_weight[0], preferred_element_type=jnp.float32)
    hidden = (jax.nn.silu(gate_value) * up_value).astype(jnp.bfloat16)
    partial = jnp.dot(hidden, down_weight[0], preferred_element_type=jnp.float32)
    partial = partial.astype(jnp.bfloat16).reshape(d, rows, width)
    probe_out = back(partial, sources, n)
    return (expert_load, expert_energy, probe_out)


def solution(mesh):
    in_specs = (
        P(("dp", "expert"), None),
        P(("dp", "expert"), None),
        P(),
        P("expert", None, "dp"),
        P("expert", None, "dp"),
        P("expert", "dp", None),
        P(),
        P(),
        P(("dp", "expert")),
    )
    out_specs = (P("expert"), P("expert"), P(("dp", "expert"), None))
    return jax.shard_map(
        on_device, mesh=mesh, in_specs=in_specs, out_specs=out_specs, check_vma=False
    )
```

```python
import functools

import jax
import jax.numpy as jnp
from jax import lax
from jax.experimental import pallas as pl
from jax.experimental.pallas import tpu as pltpu
from jax.sharding import PartitionSpec as P

EXP_DEV = 8
LANES = 128
MESH = pl.DeviceIdType.MESH
VMEM = pl.BlockSpec(memory_space=pltpu.VMEM)
SMEM = pl.BlockSpec(memory_space=pltpu.SMEM)
epsilon = 1e-06


def piece_width(width, n):
    w = LANES * -(-width // (LANES * n))
    while width % w:
        w += LANES
    return w


def prepare_kernel(routed, ids, probe, gain, normed, stats):
    tokens, width = routed.shape
    experts = stats.shape[1]
    total = jnp.zeros((tokens, LANES), jnp.float32)
    for c in range(width // LANES):
        x = routed[:, c * LANES : (c + 1) * LANES].astype(jnp.float32)
        total = total + x * x
    mean_square = jnp.sum(total, axis=1, keepdims=True) / width
    lane = lax.broadcasted_iota(jnp.int32, (tokens, experts), 1)
    chosen = jnp.zeros((tokens, experts), jnp.float32)
    for k in range(ids.shape[1]):
        chosen = chosen + jnp.where(ids[:, k : k + 1] == lane, 1.0, 0.0)
    stats[...] = jnp.zeros_like(stats)
    stats[0:1, :] = jnp.sum(chosen, axis=0, keepdims=True)
    stats[1:2, :] = jnp.sum(chosen * mean_square, axis=0, keepdims=True)
    probes = probe.shape[0]
    row = lax.broadcasted_iota(jnp.int32, (tokens, tokens), 0)
    column = lax.broadcasted_iota(jnp.int32, (tokens, tokens), 1)
    flat = jnp.sum(jnp.where(row == column, mean_square, 0.0), axis=0, keepdims=True)
    pick = probe[...] == lax.broadcasted_iota(jnp.int32, (probes, tokens), 1)
    scale = lax.rsqrt(jnp.sum(jnp.where(pick, flat, 0.0), axis=1, keepdims=True) + epsilon)
    pick = jnp.where(pick, 1.0, 0.0).astype(jnp.bfloat16)
    step = 512 if width % 512 == 0 else LANES
    for c in range(width // step):
        cols = slice(c * step, (c + 1) * step)
        rows = jnp.dot(pick, routed[:, cols], preferred_element_type=jnp.float32)
        normed[:, cols] = (rows * scale * gain[:, cols].astype(jnp.float32)).astype(jnp.bfloat16)


def prepare(routed, expert_ids, probe_ids, norm_gain, experts):
    probes = probe_ids.shape[0]
    width = routed.shape[1]
    return pl.pallas_call(
        prepare_kernel,
        out_shape=(
            jax.ShapeDtypeStruct((probes, width), jnp.bfloat16),
            jax.ShapeDtypeStruct((8, experts), jnp.float32),
        ),
        in_specs=[VMEM] * 4,
        out_specs=(VMEM, VMEM),
        compiler_params=pltpu.CompilerParams(vmem_limit_bytes=16 << 20),
        cost_estimate=pl.CostEstimate(flops=10**8, bytes_accessed=3 << 20, transcendentals=0),
    )(routed, expert_ids, probe_ids.reshape(probes, 1), norm_gain.reshape(1, width))


def remote(src, dst, send, recv, device):
    return pltpu.make_async_remote_copy(
        src_ref=src, dst_ref=dst, send_sem=send, recv_sem=recv, device_id=device, device_id_type=MESH
    )


def greet(g, me, d, n):
    barrier = pltpu.get_barrier_semaphore()
    for k in range(1, n):
        pl.semaphore_signal(barrier, inc=1, device_id=(g, lax.rem(me + k, n)), device_id_type=MESH)
    for c in range(1, d):
        pl.semaphore_signal(barrier, inc=1, device_id=(lax.rem(g + c, d), me), device_id_type=MESH)
    pl.semaphore_wait(barrier, n - 1 + d - 1)


class Pieces:
    def __init__(self, width, n):
        self.n = n
        self.w = piece_width(width, n)
        self.count = width // self.w

    def of(self, i):
        p = (i * self.count + self.n - 1) // self.n
        return jnp.minimum(p, self.count - 1), (p < self.count) & ((p * self.n) // self.count == i)

    def cols(self, p):
        return pl.ds(pl.multiple_of(p * self.w, self.w), self.w)


def fused_kernel(d, n, lag, source, home, normed, stats, gate_hbm, up_hbm, down_hbm, out, totals,
                 wg, wu, wd, x, gate_sum, up_sum, hidden, partial, arrived, summed, relay, outbox, relay2, outbox2,
                 st_in, st_mid, st_dp, sw, sd, s1, r1, s2, r2, sy, ry, ss, rs, ssy, rsy, s3, r3, s4, r4, sz, rz):
    g, me = lax.axis_index("dp"), lax.axis_index("expert")
    rows, width = normed.shape
    pieces = Pieces(width, n)
    mine, relays = pieces.of(me)
    count = pieces.count
    tall = d * rows
    down_step = wd.shape[0] // sd.shape[0]

    loads = []
    for p in range(count):
        part = pl.ds(p * pieces.w, pieces.w)
        loads.append(pltpu.make_async_copy(gate_hbm.at[part, :], wg.at[part, :], sw.at[0, p]))
        loads.append(pltpu.make_async_copy(up_hbm.at[part, :], wu.at[part, :], sw.at[1, p]))
    for p in range(sd.shape[0]):
        part = pl.ds(p * down_step, down_step)
        loads.append(pltpu.make_async_copy(down_hbm.at[part, :], wd.at[part, :], sd.at[p]))
    for load in loads:
        load.start()
    greet(g, me, d, n)

    def first(k):
        t = lax.rem(me + k, n)
        p, ok = pieces.of(t)
        return remote(normed.at[:, pieces.cols(p)], relay.at[me], s1.at[k], r1.at[me], (g, t)), ok

    def first_in(k):
        s = lax.rem(me + n - k, n)
        return remote(normed.at[:, pieces.cols(mine)], relay.at[s], s1.at[k], r1.at[s], (g, s))

    def stat(k):
        t = lax.rem(me + k, n)
        return remote(stats, st_in.at[me], ss.at[k], rs.at[me], (g, t))

    def stat_in(k):
        s = lax.rem(me + n - k, n)
        return remote(stats, st_in.at[s], ss.at[k], rs.at[s], (g, s))

    def second(k):
        j = lax.rem(me + k, n)
        return remote(outbox.at[j], x.at[g, :, pieces.cols(mine)], s2.at[k], r2.at[mine], (g, j))

    def along(p, c):
        here = x.at[g, :, pieces.cols(p)]
        return remote(here, here, sy.at[c, p], ry.at[g, p], (lax.rem(g + c, d), me))

    for k in range(1, n):
        copy, ok = first(k)
        pl.when(ok)(copy.start)
    for k in range(1, n):
        stat(k).start()
    st_in[me] = stats[...]
    gate_sum[...] = jnp.zeros_like(gate_sum)
    up_sum[...] = jnp.zeros_like(up_sum)

    @pl.when(relays)
    def _():
        relay[me] = normed[:, pieces.cols(mine)]
        for k in range(1, n):
            first_in(k).wait_recv()
        for k in range(1, n):
            j = lax.rem(me + k, n)
            outbox[j] = relay[source[j]]
            second(k).start()
        x[g, :, pieces.cols(mine)] = relay[source[me]]

    for load in loads:
        load.wait()

    def take(k):
        i = lax.rem(me + n - k, n)
        p, ok = pieces.of(i)

        @pl.when(ok)
        def _():
            @pl.when(k > 0)
            def _():
                remote(outbox.at[i], x.at[g, :, pieces.cols(p)], s2.at[k], r2.at[p], (g, i)).wait_recv()
            for c in range(1, d):
                along(p, c).start()

    def absorb(k):
        p, ok = pieces.of(lax.rem(me + n - k, n))

        @pl.when(ok)
        def _():
            for c in range(1, d):
                f = lax.rem(g + d - c, d)
                there = x.at[f, :, pieces.cols(p)]
                remote(there, there, sy.at[c, p], ry.at[f, p], (f, me)).wait_recv()
            part = x[:, :, pieces.cols(p)].astype(jnp.float32).reshape(tall, pieces.w).astype(jnp.bfloat16)
            gate_sum[...] += jnp.dot(part, wg[pieces.cols(p), :], preferred_element_type=jnp.float32)
            up_sum[...] += jnp.dot(part, wu[pieces.cols(p), :], preferred_element_type=jnp.float32)

    for k in range(lag):
        take(k)

    @pl.loop(lag, n)
    def _(k):
        take(k)
        absorb(k - lag)

    @pl.loop(n - lag, n)
    def _(k):
        absorb(k)

    gate = gate_sum[...]
    hidden[...] = (gate / (1.0 + jnp.exp(-gate)) * up_sum[...]).astype(jnp.bfloat16)

    def home_copy(p, c):
        t = lax.rem(g + c, d)
        return remote(partial.at[p, t], arrived.at[g, p], sz.at[c, p], rz.at[g, p], (t, me))

    def third(p, k, t):
        return remote(summed.at[p], relay2.at[me], s3.at[k], r3.at[me], (g, t))

    def fourth(k):
        j = lax.rem(me + k, n)
        return remote(outbox2.at[j], out.at[:, pieces.cols(mine)], s4.at[k], r4.at[mine], (g, j))

    def make(k):
        p, ok = pieces.of(lax.rem(me + k, n))

        @pl.when(ok)
        def _():
            value = jnp.dot(hidden[...], wd[:, pieces.cols(p)], preferred_element_type=jnp.float32)
            partial[p] = value.reshape(d, rows, pieces.w).astype(jnp.bfloat16)
            for c in range(1, d):
                home_copy(p, c).start()

    def add(k):
        t = lax.rem(me + k, n)
        p, ok = pieces.of(t)

        @pl.when(ok)
        def _():
            for c in range(1, d):
                f = lax.rem(g + d - c, d)
                remote(partial.at[p, f], arrived.at[f, p], sz.at[c, p], rz.at[f, p], (f, me)).wait_recv()
            arrived[g, p] = partial[p, g]
            total = arrived[0, p].astype(jnp.float32)
            for f in range(1, d):
                total = total + arrived[f, p].astype(jnp.float32)

            @pl.when(t != me)
            def _():
                summed[p] = total.astype(jnp.bfloat16)
                third(p, k, t).start()

            @pl.when(t == me)
            def _():
                relay2[me] = total.astype(jnp.bfloat16)

    @pl.loop(1, lag + 1)
    def _(k):
        make(k)

    @pl.loop(lag + 1, n + 1)
    def _(k):
        make(k)
        add(k - lag)

    @pl.loop(n + 1 - lag, n + 1)
    def _(k):
        add(k)

    for k in range(1, n):
        stat_in(k).wait_recv()
    mid = st_in[0]
    for s in range(1, n):
        mid = mid + st_in[s]
    st_mid[...] = mid
    st_dp[g] = mid
    for c in range(1, d):
        remote(st_mid, st_dp.at[g], ssy.at[c], rsy.at[g], (lax.rem(g + c, d), me)).start()

    @pl.when(relays)
    def _():
        for k in range(1, n):
            s = lax.rem(me + n - k, n)
            remote(summed.at[mine], relay2.at[s], s3.at[k], r3.at[s], (g, s)).wait_recv()
        for k in range(1, n):
            j = lax.rem(me + k, n)
            outbox2[j] = relay2[home[j]]
            fourth(k).start()
        out[:, pieces.cols(mine)] = relay2[home[me]]

    for c in range(1, d):
        f = lax.rem(g + d - c, d)
        remote(st_mid, st_dp.at[f], ssy.at[c], rsy.at[f], (f, me)).wait_recv()
    total = st_dp[0]
    for f in range(1, d):
        total = total + st_dp[f]
    totals[...] = total

    for k in range(1, n):
        copy, ok = first(k)
        pl.when(ok)(copy.wait_send)
        stat(k).wait_send()
    for c in range(1, d):
        remote(st_mid, st_dp.at[g], ssy.at[c], rsy.at[g], (lax.rem(g + c, d), me)).wait_send()
        for p in range(count):
            along(p, c).wait_send()
            home_copy(p, c).wait_send()
    for k in range(1, n):
        t = lax.rem(me + k, n)
        p, ok = pieces.of(t)
        pl.when(ok)(third(p, k, t).wait_send)

    @pl.when(relays)
    def _():
        for k in range(1, n):
            second(k).wait_send()
            fourth(k).wait_send()

    for k in range(1, n):
        i = lax.rem(me + n - k, n)
        p, ok = pieces.of(i)

        @pl.when(ok)
        def _():
            remote(outbox2.at[i], out.at[:, pieces.cols(p)], s4.at[k], r4.at[p], (g, i)).wait_recv()


def fused(normed, stats, source, home, gate, up, down, d, n):
    rows, width = normed.shape
    pieces = Pieces(width, n)
    units = gate.shape[1]
    count, w = pieces.count, pieces.w
    dma = pltpu.SemaphoreType.DMA
    block = lambda *shape: pltpu.VMEM(shape, jnp.bfloat16)
    wide = lambda *shape: pltpu.VMEM(shape, jnp.float32)
    anywhere = pl.BlockSpec(memory_space=pltpu.HBM)
    return pl.pallas_call(
        functools.partial(fused_kernel, d, n, 4),
        out_shape=(
            jax.ShapeDtypeStruct((rows, width), jnp.bfloat16),
            jax.ShapeDtypeStruct(stats.shape, jnp.float32),
        ),
        in_specs=[SMEM, SMEM, VMEM, VMEM, anywhere, anywhere, anywhere],
        out_specs=(VMEM, VMEM),
        scratch_shapes=[
            block(width, units), block(width, units), block(units, width),
            block(d, rows, width),
            wide(d * rows, units), wide(d * rows, units), block(d * rows, units),
            block(count, d, rows, w), block(d, count, rows, w), block(count, rows, w),
            block(n, rows, w), block(n, rows, w), block(n, rows, w), block(n, rows, w),
            wide(n, *stats.shape), wide(*stats.shape), wide(d, *stats.shape),
            dma((2, count)), dma((8,)),
            dma((n,)), dma((n,)), dma((n,)), dma((count,)), dma((d, count)), dma((d, count)),
            dma((n,)), dma((n,)), dma((d,)), dma((d,)),
            dma((n,)), dma((n,)), dma((n,)), dma((count,)), dma((d, count)), dma((d, count)),
        ],
        compiler_params=pltpu.CompilerParams(
            collective_id=0, has_side_effects=True, vmem_limit_bytes=62 << 20
        ),
    )(source, home, normed, stats, gate, up, down)


def on_device(
    routed,
    expert_ids,
    norm_gain,
    gate_weight,
    up_weight,
    down_weight,
    old_place,
    new_place,
    probe_ids,
):
    n, d = lax.axis_size("expert"), lax.axis_size("dp")
    experts = EXP_DEV * n
    tokens = routed.shape[0] * d * n
    normed, stats = prepare(routed, expert_ids, probe_ids, norm_gain, experts)
    slot_index = jnp.arange(n, dtype=jnp.int32)
    matches = new_place[:, None] == old_place[None, :]
    sources = jnp.sum(jnp.where(matches, slot_index[None, :], 0), axis=1)
    targets = jnp.sum(jnp.where(matches, slot_index[:, None], 0), axis=0)
    probe_out, totals = fused(
        normed, stats, targets, sources, gate_weight[0], up_weight[0], down_weight[0], d, n
    )
    owned = lax.dynamic_slice_in_dim(totals, lax.axis_index("expert") * EXP_DEV, EXP_DEV, 1)
    expert_load = owned[0] * experts / (tokens * expert_ids.shape[1])
    expert_energy = owned[1] / owned[0]
    return (expert_load, expert_energy, probe_out)


def solution(mesh):
    in_specs = (
        P(("dp", "expert"), None),
        P(("dp", "expert"), None),
        P(),
        P("expert", None, "dp"),
        P("expert", None, "dp"),
        P("expert", "dp", None),
        P(),
        P(),
        P(("dp", "expert")),
    )
    out_specs = (P("expert"), P("expert"), P(("dp", "expert"), None))
    return jax.shard_map(
        on_device, mesh=mesh, in_specs=in_specs, out_specs=out_specs, check_vma=False
    )
```
